32 devices in a mesh: dp: 32 (over z, y, x, core).
Axes of the slice: x: 2, y: 2, z: 4, core: 2. Of those that a mesh axis runs over, the one named last changes fastest.
Arguments:
- img_emb: bfloat16 [16384, 1280], P('dp')
- txt_emb: bfloat16 [16384, 1280], P('dp')
- log_temp: float32 [], replicated
- logit_bias: float32 [], replicated
Outputs:
- output 1: float32 [], replicated
- output 2: float32 [16384, 1280], P('dp')
- output 3: float32 [16384, 1280], P('dp')
- output 4: float32 [], replicated
- output 5: float32 [], replicated
All inputs are finite; a program needn't handle non-finite values.
Results may differ from the reference program's by a relative error of at most 0.001.
Values are sent between devices in bfloat16 or wider.
A program may use at most 1 GiB of HBM per device.

```python
import jax
import jax.numpy as jnp
from jax import lax

EMBED_DIM = 1280
ROWS_DEV = 512
GROUP_SIZE = 32


def setup_inputs(seed: int = 0) -> dict:
    total_rows = ROWS_DEV * GROUP_SIZE
    num_groups = total_rows // 4
    unit_scale = EMBED_DIM ** -0.5
    rand_keys = jax.random.split(jax.random.key(seed), 10)
    shared_dir = jax.random.normal(rand_keys[0], (EMBED_DIM,), jnp.float32) * unit_scale
    centers = jax.random.normal(rand_keys[1], (num_groups, EMBED_DIM), jnp.float32) * unit_scale
    member = jax.random.randint(rand_keys[2], (total_rows,), 0, num_groups)
    own_part = jax.random.normal(rand_keys[3], (total_rows, EMBED_DIM), jnp.float32) * unit_scale
    img_noise = jax.random.normal(rand_keys[4], (total_rows, EMBED_DIM), jnp.float32) * unit_scale
    txt_noise = jax.random.normal(rand_keys[5], (total_rows, EMBED_DIM), jnp.float32) * unit_scale
    common = 0.47 * centers[member] + 0.28 * own_part
    img_scale = jax.random.uniform(rand_keys[6], (total_rows, 1), jnp.float32, minval=20.0, maxval=60.0)
    txt_scale = jax.random.uniform(rand_keys[7], (total_rows, 1), jnp.float32, minval=20.0, maxval=60.0)
    img_emb = (img_scale * (0.35 * shared_dir + common + 0.76 * img_noise)).astype(jnp.bfloat16)
    txt_emb = (txt_scale * (common - 0.35 * shared_dir + 0.76 * txt_noise)).astype(jnp.bfloat16)
    log_temp = jax.random.uniform(rand_keys[8], (), jnp.float32, minval=4.6, maxval=4.8)
    logit_bias = jax.random.uniform(rand_keys[9], (), jnp.float32, minval=-14.0, maxval=-10.0)
    return {"img_emb": img_emb, "txt_emb": txt_emb, "log_temp": log_temp, "logit_bias": logit_bias}


def normalize_rows(emb):
    emb32 = emb.astype(jnp.float32)
    inv_norm = lax.rsqrt(jnp.sum(emb32 * emb32, axis=-1, keepdims=True))
    return emb32 * inv_norm, inv_norm


def project_back(unit_rows, inv_norm, grad_dir):
    radial = jnp.sum(unit_rows * grad_dir, axis=-1, keepdims=True)
    return (grad_dir - unit_rows * radial) * inv_norm


def reference(img_emb, txt_emb, log_temp, logit_bias):
    total_rows = img_emb.shape[0]
    embed_width = img_emb.shape[1]
    block_rows = min(ROWS_DEV, 512)
    num_blocks = total_rows // block_rows
    img_unit, img_inv = normalize_rows(img_emb)
    txt_unit, txt_inv = normalize_rows(txt_emb)
    img_b = img_unit.astype(jnp.bfloat16)
    txt_b = txt_unit.astype(jnp.bfloat16)
    temp_scale = jnp.exp(log_temp)
    col_ids = jnp.arange(total_rows)

    def row_block(acc_state, block_in):
        x_blk, blk_idx = block_in
        loss_sum, weight_sum, weighted_sim, txt_grad = acc_state
        sim_vals = jnp.dot(x_blk, txt_b.T, preferred_element_type=jnp.float32)
        logits = temp_scale * sim_vals + logit_bias
        row_ids = blk_idx * block_rows + jnp.arange(block_rows)
        label_signs = jnp.where(row_ids[:, None] == col_ids[None, :], 1.0, -1.0)
        weights = -label_signs * jax.nn.sigmoid(-label_signs * logits)
        weights_b = weights.astype(jnp.bfloat16)
        new_state = (
            loss_sum + jnp.sum(jax.nn.softplus(-label_signs * logits)),
            weight_sum + jnp.sum(weights),
            weighted_sim + jnp.sum(weights * sim_vals),
            txt_grad + jnp.dot(weights_b.T, x_blk, preferred_element_type=jnp.float32),
        )
        return new_state, jnp.dot(weights_b, txt_b, preferred_element_type=jnp.float32)

    init_state = (
        jnp.zeros((), jnp.float32),
        jnp.zeros((), jnp.float32),
        jnp.zeros((), jnp.float32),
        jnp.zeros((total_rows, embed_width), jnp.float32),
    )
    blocks_in = (img_b.reshape(num_blocks, block_rows, embed_width), jnp.arange(num_blocks))
    final_state, img_parts = lax.scan(row_block, init_state, blocks_in)
    loss_sum, weight_sum, weighted_sim, txt_grad = final_state
    img_dir = temp_scale * img_parts.reshape(total_rows, embed_width)
    txt_dir = temp_scale * txt_grad
    loss_val = loss_sum / total_rows
    grad_img = project_back(img_unit, img_inv, img_dir)
    grad_txt = project_back(txt_unit, txt_inv, txt_dir)
    grad_log_temp = temp_scale * weighted_sim / total_rows
    grad_bias = weight_sum / total_rows
    return (loss_val, grad_img, grad_txt, grad_log_temp, grad_bias)
```

```python
import jax
import jax.numpy as jnp
from jax import lax
from jax.sharding import PartitionSpec as P


def normalize_rows(emb):
    emb32 = emb.astype(jnp.float32)
    inv_norm = lax.rsqrt(jnp.sum(emb32 * emb32, axis=-1, keepdims=True))
    return emb32 * inv_norm, inv_norm


def project_back(unit_rows, inv_norm, grad_dir):
    radial = jnp.sum(unit_rows * grad_dir, axis=-1, keepdims=True)
    return (grad_dir - unit_rows * radial) * inv_norm


def solution(mesh):
    n_dev = mesh.shape['dp']
    plane = 8
    n_z = n_dev // plane
    col_groups = [[b + plane * z for z in range(n_z)] for b in range(plane)]
    row_groups = [[z * plane + b for b in range(plane)] for z in range(n_z)]

    def local_fn(img_emb, txt_emb, log_temp, logit_bias):
        rows = img_emb.shape[0]
        total_rows = rows * n_dev
        me = lax.axis_index('dp')
        img_unit, img_inv = normalize_rows(img_emb)
        txt_unit, txt_inv = normalize_rows(txt_emb)
        temp_scale = jnp.exp(log_temp)
        xs = lax.all_gather(img_unit.astype(jnp.bfloat16), 'dp', axis_index_groups=col_groups, tiled=True)
        ys = lax.all_gather(txt_unit.astype(jnp.bfloat16), 'dp', axis_index_groups=row_groups, tiled=True)
        i = jnp.arange(xs.shape[0])
        j = jnp.arange(ys.shape[0])
        gi = (i // rows * plane + me % plane) * rows + i % rows
        gj = (me // plane) * plane * rows + j
        sim = jnp.einsum('id,jd->ij', xs, ys, preferred_element_type=jnp.float32)
        logits = temp_scale * sim + logit_bias
        sign = jnp.where(gi[:, None] == gj[None, :], 1.0, -1.0)
        weights = -sign * jax.nn.sigmoid(-sign * logits)
        wb = weights.astype(jnp.bfloat16)
        u = jnp.einsum('ij,jd->id', wb, ys, preferred_element_type=jnp.float32)
        v = jnp.einsum('ij,id->jd', wb, xs, preferred_element_type=jnp.float32)
        stats = jnp.stack([jnp.sum(jax.nn.softplus(-sign * logits)), jnp.sum(weights), jnp.sum(weights * sim)])
        u = lax.psum_scatter(u, 'dp', scatter_dimension=0, axis_index_groups=col_groups, tiled=True)
        v = lax.psum_scatter(v, 'dp', scatter_dimension=0, axis_index_groups=row_groups, tiled=True)
        stats = lax.psum(stats, 'dp') / total_rows
        grad_img = project_back(img_unit, img_inv, temp_scale * u)
        grad_txt = project_back(txt_unit, txt_inv, temp_scale * v)
        return stats[0], grad_img, grad_txt, temp_scale * stats[2], stats[1]

    return jax.shard_map(
        local_fn,
        mesh=mesh,
        in_specs=(P('dp', None), P('dp', None), P(), P()),
        out_specs=(P(), P('dp', None), P('dp', None), P(), P()),
        check_vma=False,
    )
```

```python
import functools
import math

import jax
import jax.numpy as jnp
from jax import lax
from jax.experimental import pallas as pl
from jax.experimental.pallas import tpu as pltpu
from jax.sharding import PartitionSpec as P

F32 = jnp.float32
BF16 = jnp.bfloat16
MESH = pl.DeviceIdType.MESH
LOG2E = math.log2(math.e)
LN2 = math.log(2.0)
PLANE = 8
RING = 4
PIECES = 2


def dot_f32(lhs, rhs, lhs_dim, rhs_dim):
    return lax.dot_general(lhs, rhs, (((lhs_dim,), (rhs_dim,)), ((), ())), preferred_element_type=F32)


def pick(table, idx):
    out = jnp.int32(table[0])
    for pos in range(1, len(table)):
        out = jnp.where(idx == pos, jnp.int32(table[pos]), out)
    return out


def loss_kernel(scal, img_hbm, txt_hbm, u_out, v_out, stat_out,
                X, Y, H, PU, RU, DV, WV, RV, ST, SE,
                ld_sem, gx_s, gx_r, gy_s, gy_r, yd_s, yd_r, ru_s, ru_r, rv_s, rv_r,
                dv_s, dv_r, se_s, se_r, out_sem, credit):
    rows, width = img_hbm.shape
    half = rows // 2
    piece = half // PIECES
    me = lax.axis_index('dp')
    z = me // PLANE
    rem = me % PLANE
    y = rem // 4
    x = (rem // 2) % 2
    core = rem % 2
    q = 2 * y + (x + y - 2 * x * y)

    def z_dev(step):
        return ((z + step) % RING) * PLANE + rem

    def q_dev(step):
        q2 = (q + step) % RING
        y2 = q2 // 2
        b2 = q2 % 2
        x2 = b2 + y2 - 2 * b2 * y2
        return z * PLANE + y2 * 4 + x2 * 2 + core

    partner = me + 1 - 2 * core
    z_peers = [z_dev(k) for k in range(1, RING)]
    plane_peers = [z * PLANE + (rem + k) % PLANE for k in range(1, PLANE)]

    barrier = pltpu.get_barrier_semaphore()
    for dev in z_peers + plane_peers:
        pl.semaphore_signal(barrier, inc=1, device_id=(dev,), device_id_type=MESH)

    ld_x = pltpu.make_async_copy(img_hbm, X.at[pl.ds(0, rows)], ld_sem.at[0])
    ld_y = pltpu.make_async_copy(txt_hbm, Y.at[pl.ds(0, rows)], ld_sem.at[1])
    ld_x.start()
    ld_y.start()
    ST[...] = jnp.zeros_like(ST)

    def normalize(ref):
        blk = min(64, rows)

        def body(k, carry):
            sl = pl.ds(pl.multiple_of(k * blk, blk), blk)
            e32 = ref[sl, :].astype(F32)
            ref[sl, :] = (e32 * lax.rsqrt(jnp.sum(e32 * e32, axis=-1, keepdims=True))).astype(BF16)
            return carry

        lax.fori_loop(0, rows // blk, body, 0)

    def xrow(g, h=0):
        return g * rows + h * half

    def yrow(g, h=0, other=0):
        return g * 2 * rows + other * rows + h * half

    def remote(src, dst, ss, rs, dev):
        return pltpu.make_async_remote_copy(src_ref=src, dst_ref=dst, send_sem=ss, recv_sem=rs,
                                            device_id=(dev,), device_id_type=MESH)

    moves = [((0, 0), (1, 0), 1), ((0, 1), (1, 1), -1), ((0, 1), (2, 1), 1), ((0, 0), (2, 0), -1),
             ((1, 0), (3, 0), 1), ((1, 1), (3, 1), -1)]
    gx = []
    gy = []
    for n, (src, dst, step) in enumerate(moves):
        gx.append(remote(X.at[pl.ds(xrow(*src), half)], X.at[pl.ds(xrow(*dst), half)],
                         gx_s.at[n], gx_r.at[n], z_dev(step)))
        gy.append(remote(Y.at[pl.ds(yrow(*src), half)], Y.at[pl.ds(yrow(*dst), half)],
                         gy_s.at[n], gy_r.at[n], q_dev(step)))
    arrival = {dst: n for n, (_, dst, _) in enumerate(moves)}
    yd = {}
    for g in range(RING):
        for h in range(2):
            n = 2 * g + h
            yd[g, h] = remote(Y.at[pl.ds(yrow(g, h), half)], Y.at[pl.ds(yrow(g, h, 1), half)],
                              yd_s.at[n], yd_r.at[n], partner)

    temp2 = scal[0] * LOG2E
    bias2 = scal[1] * LOG2E

    def col_sum(val):
        return jnp.sum(val.reshape(val.shape[0] // 8, 8, val.shape[1]), axis=0)

    def logits_tile(gi, gj, other, diag):
        jrow = pl.multiple_of(gj * (2 * rows) + other * rows, rows)
        for h in range(2):
            logits_half(pl.multiple_of(gi * rows + h * half, half), jrow, h * half if diag else None)

    def logits_half(irow, jrow, shift):
        sim = dot_f32(X[pl.ds(irow, half), :], Y[pl.ds(jrow, rows), :], 1, 1)
        lg = sim * temp2 + bias2
        ex = jnp.exp2(-jnp.abs(lg))
        rc = 1.0 / (1.0 + ex)
        er = ex * rc
        wt = jnp.where(lg >= 0.0, rc, er)
        ramp = jnp.maximum(lg, 0.0)
        if shift is not None:
            same = (lax.broadcasted_iota(jnp.int32, sim.shape, 0) + shift
                    == lax.broadcasted_iota(jnp.int32, sim.shape, 1))
            wt = jnp.where(same, -jnp.where(lg >= 0.0, er, rc), wt)
            ramp = jnp.where(same, jnp.maximum(-lg, 0.0), ramp)
        H[pl.ds(irow, half), pl.ds(jrow, rows)] = wt.astype(BF16)
        ST[0] += col_sum(ramp)
        ST[1] += col_sum(wt)
        ST[2] += col_sum(wt * sim)
        prod = ex
        while prod.shape[0] > 8:
            m = prod.shape[0] // 2
            a, b = prod[:m], prod[m:]
            prod = a + b + a * b
        ST[3] += jnp.log1p(prod)

    def logits_tiles(pairs):
        def body(k, carry):
            t = k // 2
            logits_tile(pick([p[0] for p in pairs], t), pick([p[1] for p in pairs], t), k % 2, False)
            return carry

        lax.fori_loop(0, 2 * len(pairs), body, 0)

    def u_sum(dst, g, lo, hi, fresh):
        if fresh:
            dst[...] = jnp.zeros(dst.shape, F32)

        def body(k, carry):
            sl = pl.ds(pl.multiple_of(k * (2 * rows), 2 * rows), 2 * rows)
            dst[...] += dot_f32(H[pl.ds(g * rows, rows), sl], Y[sl, :], 1, 0)
            return carry

        lax.fori_loop(lo, hi, body, 0)

    def v_sum(dst, g, other, lo, hi, fresh):
        if fresh:
            dst[...] = jnp.zeros(dst.shape, F32)

        def body(k, carry):
            sl = pl.ds(pl.multiple_of(k * rows, rows), rows)
            dst[...] += dot_f32(H[sl, pl.ds(yrow(g, 0, other), rows)], X[sl, :], 0, 0)
            return carry

        lax.fori_loop(lo, hi, body, 0)

    def piece_rows(d, p):
        return pl.ds(d * half + p * piece, piece)

    def ring_copy(first, slots, s_sem, r_sem, dev, s, d, p):
        src = first if s == 0 else slots.at[s - 1]
        n = (s * 2 + d) * PIECES + p
        return remote(src.at[piece_rows(d, p)], slots.at[s, piece_rows(d, p)],
                      s_sem.at[n], r_sem.at[n], dev(1 - 2 * d))

    def u_copy(s, d, p):
        return ring_copy(PU.at[0], RU, ru_s, ru_r, z_dev, s, d, p)

    def v_copy(s, d, p):
        return ring_copy(DV.at[0], RV, rv_s, rv_r, q_dev, s, d, p)

    def serve(copy, slots, part, s, p):
        for d in range(2):
            copy(s - 1, d, p).wait_recv()
            slots[s - 1, piece_rows(d, p), :] += part[piece_rows(d, p), :]
        for d in range(2):
            copy(s, d, p).start()

    def d_copy(s):
        return remote(WV, DV.at[s % 2], dv_s.at[s], dv_r.at[s], partner)

    ld_x.wait()
    normalize(X)
    ld_y.wait()
    normalize(Y)
    pl.semaphore_wait(barrier, len(z_peers) + len(plane_peers))
    for n in range(4):
        gx[n].start()
        gy[n].start()
    for h in range(2):
        yd[0, h].start()
    logits_tile(0, 0, 0, True)
    for h in range(2):
        yd[0, h].wait_recv()
    logits_tile(0, 0, 1, False)

    def land(g):
        for h in range(2):
            n = arrival[g, h]
            gx[n].wait_recv()
            if g == 1:
                gx[n + 4].start()
            gy[n].wait_recv()
            if g == 1:
                gy[n + 4].start()
            yd[g, h].start()

    def land_other(g):
        for h in range(2):
            yd[g, h].wait_recv()

    land(1)
    land_other(1)
    logits_tiles([(0, 1), (1, 0), (1, 1)])
    u_sum(PU.at[0], 1, 0, 2, True)
    v_sum(WV, 1, 1, 0, 2, True)
    land(2)
    land_other(2)
    logits_tiles([(1, 2), (2, 1), (0, 2), (2, 0), (2, 2)])
    u_sum(PU.at[0], 1, 2, 3, False)
    v_sum(WV, 1, 1, 2, 3, False)
    land(3)
    land_other(3)
    logits_tiles([(3, 1), (1, 3)])
    v_sum(WV, 1, 1, 3, 4, False)
    d_copy(0).start()
    u_sum(PU.at[0], 1, 3, 4, False)
    for p in range(PIECES):
        for d in range(2):
            u_copy(0, d, p).start()
    logits_tiles([(0, 3)])
    d_copy(0).wait_recv()
    v_sum(DV.at[0], 1, 0, 0, 4, False)
    for p in range(PIECES):
        for d in range(2):
            v_copy(0, d, p).start()
    logits_tiles([(2, 3), (3, 0), (3, 2), (3, 3)])

    rows_out = []
    for k in range(4):
        acc = jnp.sum(ST[k], axis=0, keepdims=True)
        tot = acc[:, :128]
        for m in range(1, acc.shape[1] // 128):
            tot = tot + acc[:, m * 128:(m + 1) * 128]
        rows_out.append(tot)
    SE[0] = jnp.concatenate(rows_out + [jnp.zeros((4, 128), F32)], axis=0)
    se_z = [remote(SE.at[0], SE.at[1 + k], se_s.at[k], se_r.at[k], dev) for k, dev in enumerate(z_peers)]
    se_p = [remote(SE.at[4], SE.at[5 + k], se_s.at[3 + k], se_r.at[3 + k], dev)
            for k, dev in enumerate(plane_peers)]

    u_sum(PU.at[1], 3, 0, 4, True)
    for c in se_z:
        c.start()
    d_copy(0).wait_send()
    v_sum(WV, 3, 1, 0, 4, True)
    d_copy(1).start()
    serve(u_copy, RU, PU.at[1], 1, 0)
    d_copy(1).wait_recv()
    v_sum(DV.at[1], 3, 0, 0, 4, False)
    serve(u_copy, RU, PU.at[1], 1, 1)
    serve(v_copy, RV, DV.at[1], 1, 0)
    for c in se_z:
        c.wait_recv()
    SE[4] = SE[0] + SE[1] + SE[2] + SE[3]
    for p in range(PIECES):
        for d in range(2):
            u_copy(0, d, p).wait_send()
    u_sum(PU.at[0], 2, 0, 4, True)
    for c in se_p:
        c.start()
    serve(v_copy, RV, DV.at[1], 1, 1)
    pl.semaphore_signal(credit.at[1], inc=1, device_id=(partner,), device_id_type=MESH)
    for p in range(PIECES):
        for d in range(2):
            v_copy(0, d, p).wait_send()
    pl.semaphore_signal(credit.at[0], inc=1, device_id=(partner,), device_id_type=MESH)
    d_copy(1).wait_send()
    v_sum(WV, 2, 1, 0, 4, True)
    pl.semaphore_wait(credit.at[0], 1)
    d_copy(2).start()
    serve(u_copy, RU, PU.at[0], 2, 0)
    d_copy(2).wait_recv()
    v_sum(DV.at[0], 2, 0, 0, 4, False)
    u_sum(PU.at[1], 0, 0, 4, True)
    serve(v_copy, RV, DV.at[0], 2, 0)
    d_copy(2).wait_send()
    v_sum(WV, 0, 1, 0, 4, True)
    pl.semaphore_wait(credit.at[1], 1)
    d_copy(3).start()
    serve(u_copy, RU, PU.at[0], 2, 1)
    d_copy(3).wait_recv()
    v_sum(DV.at[1], 0, 0, 0, 4, False)
    serve(v_copy, RV, DV.at[0], 2, 1)
    for n in range(6):
        gx[n].wait_send()
        gy[n].wait_send()
    for g in range(RING):
        for h in range(2):
            yd[g, h].wait_send()
    raw_x = pltpu.make_async_copy(img_hbm, X.at[pl.ds(rows, rows)], ld_sem.at[0])
    raw_y = pltpu.make_async_copy(txt_hbm, X.at[pl.ds(2 * rows, rows)], ld_sem.at[1])
    raw_x.start()
    raw_y.start()
    for c in se_p:
        c.wait_recv()
    total = SE[4]
    for k in range(7):
        total = total + SE[5 + k]
    stat_out[...] = jnp.broadcast_to(jnp.sum(total, axis=1, keepdims=True), stat_out.shape)
    raw_x.wait()
    raw_y.wait()
    temp = scal[0]

    def finish(copy, slots, part, raw_row, out, d, p, sem):
        copy(2, d, p).wait_recv()
        blk = min(32, piece)

        def body(k, carry):
            at = d * half + p * piece + k * blk
            sl = pl.ds(pl.multiple_of(at, blk), blk)
            e32 = X[pl.ds(pl.multiple_of(raw_row + at, blk), blk), :].astype(F32)
            inv = lax.rsqrt(jnp.sum(e32 * e32, axis=-1, keepdims=True))
            unit = e32 * inv
            grad = (slots[2, sl, :] + part[sl, :]) * temp
            radial = jnp.sum(unit * grad, axis=-1, keepdims=True)
            slots[2, sl, :] = (grad - unit * radial) * inv
            return carry

        lax.fori_loop(0, piece // blk, body, 0)
        return pltpu.make_async_copy(slots.at[2, piece_rows(d, p)], out.at[piece_rows(d, p)], sem)

    outs = []
    for p in range(PIECES):
        for d in range(2):
            outs.append(finish(u_copy, RU, PU.at[1], rows, u_out, d, p, out_sem.at[len(outs)]))
            outs[-1].start()
        for d in range(2):
            outs.append(finish(v_copy, RV, DV.at[1], 2 * rows, v_out, d, p, out_sem.at[len(outs)]))
            outs[-1].start()
    for s in range(1, 3):
        for p in range(PIECES):
            for d in range(2):
                u_copy(s, d, p).wait_send()
                v_copy(s, d, p).wait_send()
    d_copy(3).wait_send()
    for c in se_z + se_p:
        c.wait_send()
    for c in outs:
        c.wait()


def solution(mesh):
    n_dev = mesh.shape['dp']

    def local_fn(img_emb, txt_emb, log_temp, logit_bias):
        rows, width = img_emb.shape
        total_rows = rows * n_dev
        temp_scale = jnp.exp(log_temp)
        scal = jnp.stack([temp_scale, logit_bias])
        dma = pltpu.SemaphoreType.DMA
        any_spec = pl.BlockSpec(memory_space=pl.ANY)
        vmem = pltpu.VMEM
        grad_img, grad_txt, stats = pl.pallas_call(
            loss_kernel,
            name='siglip_pairs',
            out_shape=(jax.ShapeDtypeStruct((rows, width), F32), jax.ShapeDtypeStruct((rows, width), F32),
                       jax.ShapeDtypeStruct((8, 128), F32)),
            in_specs=[pl.BlockSpec(memory_space=pltpu.SMEM), any_spec, any_spec],
            out_specs=(any_spec, any_spec, pl.BlockSpec(memory_space=pltpu.VMEM)),
            scratch_shapes=[
                vmem((RING * rows, width), BF16),
                vmem((2 * RING * rows, width), BF16),
                vmem((RING * rows, 2 * RING * rows), BF16),
                vmem((2, rows, width), F32),
                vmem((3, rows, width), F32),
                vmem((2, rows, width), F32),
                vmem((rows, width), F32),
                vmem((3, rows, width), F32),
                vmem((4, 8, rows), F32),
                vmem((12, 8, 128), F32),
                dma((2,)), dma((6,)), dma((6,)), dma((6,)), dma((6,)), dma((8,)), dma((8,)),
                dma((6 * PIECES,)), dma((6 * PIECES,)), dma((6 * PIECES,)), dma((6 * PIECES,)),
                dma((4,)), dma((4,)), dma((10,)), dma((10,)), dma((4 * PIECES,)),
                pltpu.SemaphoreType.REGULAR((2,)),
            ],
            compiler_params=pltpu.CompilerParams(collective_id=0, has_side_effects=True,
                                                 vmem_limit_bytes=67_000_000),
        )(scal, img_emb, txt_emb)
        sums = stats[:, 0] / total_rows
        return sums[0] * LN2 + sums[3], grad_img, grad_txt, temp_scale * sums[2], sums[1]

    return jax.shard_map(
        local_fn,
        mesh=mesh,
        in_specs=(P('dp', None), P('dp', None), P(), P()),
        out_specs=(P(), P('dp', None), P('dp', None), P(), P()),
        check_vma=False,
    )
```

```python
import functools
import math

import jax
import jax.numpy as jnp
from jax import lax
from jax.experimental import pallas as pl
from jax.experimental.pallas import tpu as pltpu
from jax.sharding import PartitionSpec as P

F32 = jnp.float32
BF16 = jnp.bfloat16
MESH = pl.DeviceIdType.MESH
LOG2E = math.log2(math.e)
LN2 = math.log(2.0)
PLANE = 8
SQUARE = 4
PIECES = 4


def dot_f32(lhs, rhs, lhs_dim, rhs_dim):
    return lax.dot_general(lhs, rhs, (((lhs_dim,), (rhs_dim,)), ((), ())), preferred_element_type=F32)


def pick(table, idx):
    out = jnp.int32(table[0])
    for pos in range(1, len(table)):
        out = jnp.where(idx == pos, jnp.int32(table[pos]), out)
    return out


def loss_kernel(scal, img_hbm, txt_hbm, u_out, v_out, stat_out,
                X, Y, H, PU, RU, DV, WV, RV, ST, SE,
                ld_sem, gx_s, gx_r, gy_s, gy_r, yd_s, yd_r, ru_s, ru_r, rv_s, rv_r,
                dv_s, dv_r, se_s, se_r, out_sem, credit, uz_credit, vz_credit):
    rows, width = img_hbm.shape
    half = rows // 2
    piece = rows // PIECES
    me = lax.axis_index('dp')
    z = me // PLANE
    rem = me % PLANE
    y = rem // 4
    x = (rem // 2) % 2
    core = rem % 2
    x_dev = z * PLANE + rem + 2 - 4 * x
    y_dev = z * PLANE + rem + 4 - 8 * y
    lo_dev = (z + 1 - 2 * (z % 2)) * PLANE + rem
    hi_dev = ((z + 2) % 4) * PLANE + rem
    partner = me + 1 - 2 * core
    z_peers = [((z + k) % 4) * PLANE + rem for k in range(1, 4)]
    plane_peers = [z * PLANE + (rem + k) % PLANE for k in range(1, PLANE)]

    barrier = pltpu.get_barrier_semaphore()
    for dev in z_peers + plane_peers:
        pl.semaphore_signal(barrier, inc=1, device_id=(dev,), device_id_type=MESH)

    def xrow(g, r=0):
        return g * rows + r

    def yrow(g, r=0, other=0):
        return g * 2 * rows + (r // half) * rows + other * half + r % half

    loads = []
    for h in range(2):
        loads.append(pltpu.make_async_copy(img_hbm.at[pl.ds(h * half, half)], X.at[pl.ds(h * half, half)],
                                           ld_sem.at[h]))
        loads.append(pltpu.make_async_copy(txt_hbm.at[pl.ds(h * half, half)], Y.at[pl.ds(yrow(0, h * half), half)],
                                           ld_sem.at[2 + h]))
    for c in loads:
        c.start()
    ST[...] = jnp.zeros_like(ST)

    def normalize(ref, row):
        blk = min(64, half)

        def body(k, carry):
            sl = pl.ds(pl.multiple_of(row + k * blk, blk), blk)
            e32 = ref[sl, :].astype(F32)
            ref[sl, :] = (e32 * lax.rsqrt(jnp.sum(e32 * e32, axis=-1, keepdims=True))).astype(BF16)
            return carry

        lax.fori_loop(0, half // blk, body, 0)

    def remote(src, dst, ss, rs, dev):
        return pltpu.make_async_remote_copy(src_ref=src, dst_ref=dst, send_sem=ss, recv_sem=rs,
                                            device_id=(dev,), device_id_type=MESH)

    def gather(ref, row_of, ss, rs, flat_dev, z_dev, kind, p):
        src, dst = ((0, 1), (0, 2), (2, 3))[kind]
        n = kind * PIECES + p
        return remote(ref.at[pl.ds(row_of(src, p * piece), piece)], ref.at[pl.ds(row_of(dst, p * piece), piece)],
                      ss.at[n], rs.at[n], z_dev if kind == 1 else flat_dev)

    def gx(kind, p):
        return gather(X, xrow, gx_s, gx_r, x_dev, lo_dev, kind, p)

    def gy(kind, p):
        return gather(Y, yrow, gy_s, gy_r, y_dev, hi_dev, kind, p)

    def yd(g, h):
        return remote(Y.at[pl.ds(yrow(g, h * half), half)], Y.at[pl.ds(yrow(g, h * half, 1), half)],
                      yd_s.at[2 * g + h], yd_r.at[2 * g + h], partner)

    temp2 = scal[0] * LOG2E
    bias2 = scal[1] * LOG2E

    def col_sum(val):
        return jnp.sum(val.reshape(val.shape[0] // 8, 8, val.shape[1]), axis=0)

    def logits_tile(i, j, diag=False):
        irow = pl.multiple_of(i * half, half)
        jrow = pl.multiple_of(j * rows, rows)
        sim = dot_f32(X[pl.ds(irow, half), :], Y[pl.ds(jrow, rows), :], 1, 1)
        lg = sim * temp2 + bias2
        ex = jnp.exp2(-jnp.abs(lg))
        rc = 1.0 / (1.0 + ex)
        er = ex * rc
        wt = jnp.where(lg >= 0.0, rc, er)
        ramp = jnp.maximum(lg, 0.0)
        if diag:
            same = (lax.broadcasted_iota(jnp.int32, sim.shape, 0)
                    == lax.broadcasted_iota(jnp.int32, sim.shape, 1))
            wt = jnp.where(same, -jnp.where(lg >= 0.0, er, rc), wt)
            ramp = jnp.where(same, jnp.maximum(-lg, 0.0), ramp)
        H[pl.ds(irow, half), pl.ds(jrow, rows)] = wt.astype(BF16)
        ST[0] += col_sum(ramp)
        ST[1] += col_sum(wt)
        ST[2] += col_sum(wt * sim)
        prod = ex
        while prod.shape[0] > 8:
            m = prod.shape[0] // 2
            a, b = prod[:m], prod[m:]
            prod = a + b + a * b
        ST[3] += jnp.log1p(prod)

    def logits_tiles(pairs):
        def body(k, carry):
            logits_tile(pick([p[0] for p in pairs], k), pick([p[1] for p in pairs], k))
            return carry

        lax.fori_loop(0, len(pairs), body, 0)

    def u_sum(dst, g, h_lo, h_hi):
        def body(k, carry):
            h = h_lo + k // 4
            out = pl.ds(pl.multiple_of(h * half, half), half)
            sl = pl.ds(pl.multiple_of((k % 4) * (2 * rows), 2 * rows), 2 * rows)

            @pl.when(k % 4 == 0)
            def _():
                dst[out, :] = jnp.zeros((half, width), F32)

            dst[out, :] += dot_f32(H[pl.ds(pl.multiple_of(g * rows + h * half, half), half), sl], Y[sl, :], 1, 0)
            return carry

        lax.fori_loop(0, 4 * (h_hi - h_lo), body, 0)

    def v_sum(dst, g, other, h_lo, h_hi):
        def body(k, carry):
            h = h_lo + k // 2
            out = pl.ds(pl.multiple_of(h * half, half), half)
            sl = pl.ds(pl.multiple_of((k % 2) * (2 * rows), 2 * rows), 2 * rows)
            if other:
                @pl.when(k % 2 == 0)
                def _():
                    dst[out, :] = jnp.zeros((half, width), F32)

            cols = pl.ds(pl.multiple_of(g * 2 * rows + h * rows + other * half, half), half)
            dst[out, :] += dot_f32(H[sl, cols], X[sl, :], 0, 0)
            return carry

        lax.fori_loop(0, 2 * (h_hi - h_lo), body, 0)

    def prow(p):
        return pl.ds(p * piece, piece)

    def reduce_copy(part, slots, ss, rs, flat_dev, z_dev, kind, p):
        src = (part.at[0], part.at[2], slots.at[0])[kind]
        dst = (slots.at[0], slots.at[1], part.at[1])[kind]
        n = kind * PIECES + p
        return remote(src.at[prow(p)], dst.at[prow(p)], ss.at[n], rs.at[n], z_dev if kind == 2 else flat_dev)

    def u_copy(kind, p):
        return reduce_copy(PU, RU, ru_s, ru_r, x_dev, lo_dev, kind, p)

    def v_copy(kind, p):
        return reduce_copy(DV, RV, rv_s, rv_r, y_dev, hi_dev, kind, p)

    def serve(copy, part, slots, free, z_dev, p):
        copy(0, p).wait_recv()
        slots[0, prow(p), :] += part[1, prow(p), :]
        pl.semaphore_signal(free.at[p], inc=1, device_id=(z_dev,), device_id_type=MESH)
        pl.semaphore_wait(free.at[p], 1)
        copy(2, p).start()

    def serve_u(p):
        serve(u_copy, PU, RU, uz_credit, lo_dev, p)

    def serve_v(p):
        serve(v_copy, DV, RV, vz_credit, hi_dev, p)

    slot_of = {3: 0, 2: 1, 1: 2, 0: 0}

    def d_copy(g, h):
        return remote(WV.at[pl.ds(h * half, half)], DV.at[slot_of[g], pl.ds(h * half, half)],
                      dv_s.at[2 * g + h], dv_r.at[2 * g + h], partner)

    def v_give(g, h):
        v_sum(WV, g, 1, h, h + 1)
        d_copy(g, h).start()

    def v_take(g, h):
        d_copy(g, h).wait_recv()
        v_sum(DV.at[slot_of[g]], g, 0, h, h + 1)

    def send_pair(copy, kind, h):
        for p in (2 * h, 2 * h + 1):
            copy(kind, p).start()

    for h in range(2):
        loads[2 * h].wait()
        normalize(X, h * half)
        loads[2 * h + 1].wait()
        normalize(Y, yrow(0, h * half))
    pl.semaphore_wait(barrier, len(z_peers) + len(plane_peers))
    for p in range(PIECES):
        for kind in range(2):
            gx(kind, p).start()
            gy(kind, p).start()
    for h in range(2):
        yd(0, h).start()

    def forward(p):
        gx(1, p).wait_recv()
        gx(2, p).start()
        gy(1, p).wait_recv()
        gy(2, p).start()

    def land(g, h):
        kind = g - 1
        for p in (2 * h, 2 * h + 1):
            if kind != 1:
                gx(kind, p).wait_recv()
                gy(kind, p).wait_recv()
        yd(g, h).start()

    order = [0, 1]

    def fresh(n):
        order.append(n)
        return [(n, m) for m in order[:-1]] + [(m, n) for m in order]

    for h in range(2):
        yd(0, h).wait_recv()
    logits_tile(0, 0, True)
    logits_tile(1, 1, True)
    logits_tiles([(0, 1), (1, 0)])
    land(1, 0)
    forward(0)
    yd(1, 0).wait_recv()
    logits_tiles(fresh(2))
    land(1, 1)
    forward(1)
    land(2, 0)
    yd(1, 1).wait_recv()
    yd(2, 0).wait_recv()
    logits_tiles(fresh(3) + fresh(4))
    forward(2)
    land(3, 0)
    yd(3, 0).wait_recv()
    logits_tiles(fresh(6))
    forward(3)
    land(2, 1)
    yd(2, 1).wait_recv()
    logits_tiles(fresh(5))
    land(3, 1)
    yd(3, 1).wait_recv()
    last = fresh(7)
    first = [(6, 7), (4, 7), (7, 6), (7, 4)]
    logits_tiles(first[:1])
    u_sum(PU.at[0], 3, 0, 1)
    send_pair(u_copy, 0, 0)
    logits_tiles(first[1:])
    v_give(3, 0)
    u_sum(PU.at[1], 2, 0, 1)
    v_take(3, 0)
    send_pair(v_copy, 0, 0)
    d_copy(3, 0).wait_send()
    v_give(2, 0)
    serve_u(0)
    v_take(2, 0)
    logits_tiles([t for t in last if t not in first])
    serve_v(0)
    u_sum(PU.at[0], 3, 1, 2)
    send_pair(u_copy, 0, 1)
    v_give(3, 1)
    u_sum(PU.at[1], 2, 1, 2)
    serve_u(1)
    v_take(3, 1)
    send_pair(v_copy, 0, 1)
    d_copy(3, 1).wait_send()
    v_give(2, 1)
    serve_v(1)

    rows_out = []
    for k in range(4):
        acc = jnp.sum(ST[k], axis=0, keepdims=True)
        tot = acc[:, :128]
        for m in range(1, acc.shape[1] // 128):
            tot = tot + acc[:, m * 128:(m + 1) * 128]
        rows_out.append(tot)
    SE[0] = jnp.concatenate(rows_out + [jnp.zeros((4, 128), F32)], axis=0)
    se_z = [remote(SE.at[0], SE.at[1 + k], se_s.at[k], se_r.at[k], dev) for k, dev in enumerate(z_peers)]
    se_p = [remote(SE.at[4], SE.at[5 + k], se_s.at[3 + k], se_r.at[3 + k], dev)
            for k, dev in enumerate(plane_peers)]

    v_take(2, 1)
    u_sum(PU.at[2], 1, 0, 2)
    for c in se_z:
        c.start()
    serve_u(2)
    for h in range(2):
        send_pair(u_copy, 1, h)
    for h in range(2):
        d_copy(2, h).wait_send()
        v_give(1, h)
    for h in range(2):
        v_take(1, h)
    serve_v(2)
    for h in range(2):
        send_pair(v_copy, 1, h)
    for c in se_z:
        c.wait_recv()
    SE[4] = SE[0] + SE[1] + SE[2] + SE[3]
    for h in range(2):
        d_copy(1, h).wait_send()
    v_sum(WV, 0, 1, 0, 2)
    for c in se_p:
        c.start()
    serve_u(3)
    for p in range(PIECES):
        u_copy(0, p).wait_send()
    u_sum(PU.at[0], 0, 0, 2)
    serve_v(3)
    for p in range(PIECES):
        v_copy(0, p).wait_send()
    pl.semaphore_signal(credit, inc=1, device_id=(partner,), device_id_type=MESH)
    pl.semaphore_wait(credit, 1)
    for h in range(2):
        d_copy(0, h).start()
    for h in range(2):
        v_take(0, h)
    for p in range(PIECES):
        for kind in range(3):
            gx(kind, p).wait_send()
            gy(kind, p).wait_send()
    for g in range(4):
        for h in range(2):
            yd(g, h).wait_send()
    raw_x = pltpu.make_async_copy(img_hbm, X.at[pl.ds(rows, rows)], ld_sem.at[0])
    raw_y = pltpu.make_async_copy(txt_hbm, X.at[pl.ds(2 * rows, rows)], ld_sem.at[1])
    raw_x.start()
    raw_y.start()
    for c in se_p:
        c.wait_recv()
    total = SE[4]
    for k in range(7):
        total = total + SE[5 + k]
    stat_out[...] = jnp.broadcast_to(jnp.sum(total, axis=1, keepdims=True), stat_out.shape)
    raw_x.wait()
    raw_y.wait()
    temp = scal[0]

    def finish(copy, slots, part, raw_row, out, p, sem):
        copy(1, p).wait_recv()
        copy(2, p).wait_recv()
        blk = min(32, piece)

        def body(k, carry):
            at = p * piece + k * blk
            sl = pl.ds(pl.multiple_of(at, blk), blk)
            e32 = X[pl.ds(pl.multiple_of(raw_row + at, blk), blk), :].astype(F32)
            inv = lax.rsqrt(jnp.sum(e32 * e32, axis=-1, keepdims=True))
            unit = e32 * inv
            grad = (slots[1, sl, :] + part[1, sl, :] + part[0, sl, :]) * temp
            radial = jnp.sum(unit * grad, axis=-1, keepdims=True)
            slots[1, sl, :] = (grad - unit * radial) * inv
            return carry

        lax.fori_loop(0, piece // blk, body, 0)
        return pltpu.make_async_copy(slots.at[1, prow(p)], out.at[prow(p)], sem)

    outs = []
    for p in range(PIECES):
        outs.append(finish(u_copy, RU, PU, rows, u_out, p, out_sem.at[len(outs)]))
        outs[-1].start()
        outs.append(finish(v_copy, RV, DV, 2 * rows, v_out, p, out_sem.at[len(outs)]))
        outs[-1].start()
    for p in range(PIECES):
        for kind in (1, 2):
            u_copy(kind, p).wait_send()
            v_copy(kind, p).wait_send()
    for h in range(2):
        d_copy(0, h).wait_send()
    for c in se_z + se_p:
        c.wait_send()
    for c in outs:
        c.wait()


def solution(mesh):
    n_dev = mesh.shape['dp']

    def local_fn(img_emb, txt_emb, log_temp, logit_bias):
        rows, width = img_emb.shape
        total_rows = rows * n_dev
        temp_scale = jnp.exp(log_temp)
        scal = jnp.stack([temp_scale, logit_bias])
        dma = pltpu.SemaphoreType.DMA
        any_spec = pl.BlockSpec(memory_space=pl.ANY)
        vmem = pltpu.VMEM
        grad_img, grad_txt, stats = pl.pallas_call(
            loss_kernel,
            name='siglip_pairs',
            out_shape=(jax.ShapeDtypeStruct((rows, width), F32), jax.ShapeDtypeStruct((rows, width), F32),
                       jax.ShapeDtypeStruct((8, 128), F32)),
            in_specs=[pl.BlockSpec(memory_space=pltpu.SMEM), any_spec, any_spec],
            out_specs=(any_spec, any_spec, pl.BlockSpec(memory_space=pltpu.VMEM)),
            scratch_shapes=[
                vmem((SQUARE * rows, width), BF16),
                vmem((2 * SQUARE * rows, width), BF16),
                vmem((SQUARE * rows, 2 * SQUARE * rows), BF16),
                vmem((3, rows, width), F32),
                vmem((2, rows, width), F32),
                vmem((3, rows, width), F32),
                vmem((rows, width), F32),
                vmem((2, rows, width), F32),
                vmem((4, 8, rows), F32),
                vmem((12, 8, 128), F32),
                dma((4,)), dma((3 * PIECES,)), dma((3 * PIECES,)), dma((3 * PIECES,)), dma((3 * PIECES,)),
                dma((8,)), dma((8,)),
                dma((3 * PIECES,)), dma((3 * PIECES,)), dma((3 * PIECES,)), dma((3 * PIECES,)),
                dma((8,)), dma((8,)), dma((10,)), dma((10,)), dma((2 * PIECES,)),
                pltpu.SemaphoreType.REGULAR,
                pltpu.SemaphoreType.REGULAR((PIECES,)), pltpu.SemaphoreType.REGULAR((PIECES,)),
            ],
            compiler_params=pltpu.CompilerParams(collective_id=0, has_side_effects=True,
                                                 vmem_limit_bytes=67_000_000),
        )(scal, img_emb, txt_emb)
        sums = stats[:, 0] / total_rows
        return sums[0] * LN2 + sums[3], grad_img, grad_txt, temp_scale * sums[2], sums[1]

    return jax.shard_map(
        local_fn,
        mesh=mesh,
        in_specs=(P('dp', None), P('dp', None), P(), P()),
        out_specs=(P(), P('dp', None), P('dp', None), P(), P()),
        check_vma=False,
    )
```

```python
import functools
import math

import jax
import jax.numpy as jnp
from jax import lax
from jax.experimental import pallas as pl
from jax.experimental.pallas import tpu as pltpu
from jax.sharding import PartitionSpec as P

F32 = jnp.float32
BF16 = jnp.bfloat16
MESH = pl.DeviceIdType.MESH
LOG2E = math.log2(math.e)
LN2 = math.log(2.0)
PLANE = 8
SQUARE = 4
PIECES = 8


def dot_f32(lhs, rhs, lhs_dim, rhs_dim):
    return lax.dot_general(lhs, rhs, (((lhs_dim,), (rhs_dim,)), ((), ())), preferred_element_type=F32)


def pick(table, idx):
    out = jnp.int32(table[0])
    for pos in range(1, len(table)):
        out = jnp.where(idx == pos, jnp.int32(table[pos]), out)
    return out


def loss_kernel(scal, img_hbm, txt_hbm, u_out, v_out, stat_out,
                X, Y, H, PU, RU, DV, WV, RV, ST, SE,
                ld_sem, gx_s, gx_r, gy_s, gy_r, yd_s, yd_r, ru_s, ru_r, rv_s, rv_r,
                dv_s, dv_r, se_s, se_r, out_sem, credit, uz_credit, vz_credit):
    rows, width = img_hbm.shape
    half = rows // 2
    piece = rows // PIECES
    me = lax.axis_index('dp')
    z = me // PLANE
    rem = me % PLANE
    y = rem // 4
    x = (rem // 2) % 2
    core = rem % 2
    x_dev = z * PLANE + rem + 2 - 4 * x
    y_dev = z * PLANE + rem + 4 - 8 * y
    lo_dev = (z + 1 - 2 * (z % 2)) * PLANE + rem
    hi_dev = ((z + 2) % 4) * PLANE + rem
    partner = me + 1 - 2 * core
    z_peers = [((z + k) % 4) * PLANE + rem for k in range(1, 4)]
    plane_peers = [z * PLANE + (rem + k) % PLANE for k in range(1, PLANE)]

    barrier = pltpu.get_barrier_semaphore()
    for dev in z_peers + plane_peers:
        pl.semaphore_signal(barrier, inc=1, device_id=(dev,), device_id_type=MESH)

    def xrow(g, r=0):
        return g * rows + r

    def yrow(g, r=0, other=0):
        return g * 2 * rows + (r // half) * rows + other * half + r % half

    loads = []
    for h in range(2):
        loads.append(pltpu.make_async_copy(img_hbm.at[pl.ds(h * half, half)], X.at[pl.ds(h * half, half)],
                                           ld_sem.at[h]))
        loads.append(pltpu.make_async_copy(txt_hbm.at[pl.ds(h * half, half)], Y.at[pl.ds(yrow(0, h * half), half)],
                                           ld_sem.at[2 + h]))
    for c in loads:
        c.start()
    ST[...] = jnp.zeros_like(ST)

    def normalize(ref, row):
        blk = min(64, half)

        def body(k, carry):
            sl = pl.ds(pl.multiple_of(row + k * blk, blk), blk)
            e32 = ref[sl, :].astype(F32)
            ref[sl, :] = (e32 * lax.rsqrt(jnp.sum(e32 * e32, axis=-1, keepdims=True))).astype(BF16)
            return carry

        lax.fori_loop(0, half // blk, body, 0)

    def remote(src, dst, ss, rs, dev):
        return pltpu.make_async_remote_copy(src_ref=src, dst_ref=dst, send_sem=ss, recv_sem=rs,
                                            device_id=(dev,), device_id_type=MESH)

    def gather(ref, row_of, ss, rs, flat_dev, z_dev, kind, p):
        src, dst = ((0, 1), (0, 2), (2, 3))[kind]
        n = kind * PIECES + p
        return remote(ref.at[pl.ds(row_of(src, p * piece), piece)], ref.at[pl.ds(row_of(dst, p * piece), piece)],
                      ss.at[n], rs.at[n], z_dev if kind == 1 else flat_dev)

    def gx(kind, p):
        return gather(X, xrow, gx_s, gx_r, x_dev, lo_dev, kind, p)

    def gy(kind, p):
        return gather(Y, yrow, gy_s, gy_r, y_dev, hi_dev, kind, p)

    def yd(g, h):
        return remote(Y.at[pl.ds(yrow(g, h * half), half)], Y.at[pl.ds(yrow(g, h * half, 1), half)],
                      yd_s.at[2 * g + h], yd_r.at[2 * g + h], partner)

    temp2 = scal[0] * LOG2E
    bias2 = scal[1] * LOG2E

    def col_sum(val):
        return jnp.sum(val.reshape(val.shape[0] // 8, 8, val.shape[1]), axis=0)

    def logits_tile(i, j, diag=False):
        irow = pl.multiple_of(i * half, half)
        jrow = pl.multiple_of(j * rows, rows)
        sim = dot_f32(X[pl.ds(irow, half), :], Y[pl.ds(jrow, rows), :], 1, 1)
        lg = sim * temp2 + bias2
        ex = jnp.exp2(-jnp.abs(lg))
        rc = 1.0 / (1.0 + ex)
        er = ex * rc
        wt = jnp.where(lg >= 0.0, rc, er)
        ramp = jnp.maximum(lg, 0.0)
        if diag:
            same = (lax.broadcasted_iota(jnp.int32, sim.shape, 0)
                    == lax.broadcasted_iota(jnp.int32, sim.shape, 1))
            wt = jnp.where(same, -jnp.where(lg >= 0.0, er, rc), wt)
            ramp = jnp.where(same, jnp.maximum(-lg, 0.0), ramp)
        H[pl.ds(irow, half), pl.ds(jrow, rows)] = wt.astype(BF16)
        ST[0] += col_sum(ramp)
        ST[1] += col_sum(wt)
        ST[2] += col_sum(wt * sim)
        prod = ex
        while prod.shape[0] > 8:
            m = prod.shape[0] // 2
            a, b = prod[:m], prod[m:]
            prod = a + b + a * b
        ST[3] += jnp.log1p(prod)

    def logits_tiles(pairs):
        def body(k, carry):
            logits_tile(pick([p[0] for p in pairs], k), pick([p[1] for p in pairs], k))
            return carry

        lax.fori_loop(0, len(pairs), body, 0)

    def u_sum(dst, g, h_lo, h_hi):
        def body(k, carry):
            h = h_lo + k // 4
            out = pl.ds(pl.multiple_of(h * half, half), half)
            sl = pl.ds(pl.multiple_of((k % 4) * (2 * rows), 2 * rows), 2 * rows)

            @pl.when(k % 4 == 0)
            def _():
                dst[out, :] = jnp.zeros((half, width), F32)

            dst[out, :] += dot_f32(H[pl.ds(pl.multiple_of(g * rows + h * half, half), half), sl], Y[sl, :], 1, 0)
            return carry

        lax.fori_loop(0, 4 * (h_hi - h_lo), body, 0)

    def v_sum(dst, g, other, h_lo, h_hi):
        def body(k, carry):
            h = h_lo + k // 2
            out = pl.ds(pl.multiple_of(h * half, half), half)
            sl = pl.ds(pl.multiple_of((k % 2) * (2 * rows), 2 * rows), 2 * rows)
            if other:
                @pl.when(k % 2 == 0)
                def _():
                    dst[out, :] = jnp.zeros((half, width), F32)

            cols = pl.ds(pl.multiple_of(g * 2 * rows + h * rows + other * half, half), half)
            dst[out, :] += dot_f32(H[sl, cols], X[sl, :], 0, 0)
            return carry

        lax.fori_loop(0, 2 * (h_hi - h_lo), body, 0)

    def prow(p):
        return pl.ds(p * piece, piece)

    def reduce_copy(part, slots, ss, rs, flat_dev, z_dev, kind, p):
        src = (part.at[0], part.at[2], slots.at[0])[kind]
        dst = (slots.at[0], slots.at[1], part.at[1])[kind]
        n = kind * PIECES + p
        return remote(src.at[prow(p)], dst.at[prow(p)], ss.at[n], rs.at[n], z_dev if kind == 2 else flat_dev)

    def u_copy(kind, p):
        return reduce_copy(PU, RU, ru_s, ru_r, x_dev, lo_dev, kind, p)

    def v_copy(kind, p):
        return reduce_copy(DV, RV, rv_s, rv_r, y_dev, hi_dev, kind, p)

    def serve(copy, part, slots, free, z_dev, p):
        copy(0, p).wait_recv()
        slots[0, prow(p), :] += part[1, prow(p), :]
        pl.semaphore_signal(free.at[p], inc=1, device_id=(z_dev,), device_id_type=MESH)
        pl.semaphore_wait(free.at[p], 1)
        copy(2, p).start()

    def serve_u(p):
        serve(u_copy, PU, RU, uz_credit, lo_dev, p)

    def serve_v(p):
        serve(v_copy, DV, RV, vz_credit, hi_dev, p)

    slot_of = {3: 0, 2: 1, 1: 2, 0: 0}

    def d_copy(g, h):
        return remote(WV.at[pl.ds(h * half, half)], DV.at[slot_of[g], pl.ds(h * half, half)],
                      dv_s.at[2 * g + h], dv_r.at[2 * g + h], partner)

    def v_give(g, h):
        v_sum(WV, g, 1, h, h + 1)
        d_copy(g, h).start()

    def v_take(g, h):
        d_copy(g, h).wait_recv()
        v_sum(DV.at[slot_of[g]], g, 0, h, h + 1)

    def pieces_of(h):
        return range(h * PIECES // 2, (h + 1) * PIECES // 2)

    def send_half(copy, kind, h):
        for p in pieces_of(h):
            copy(kind, p).start()

    for h in range(2):
        loads[2 * h].wait()
        normalize(X, h * half)
        loads[2 * h + 1].wait()
        normalize(Y, yrow(0, h * half))
    pl.semaphore_wait(barrier, len(z_peers) + len(plane_peers))
    for p in range(PIECES):
        for kind in range(2):
            gx(kind, p).start()
            gy(kind, p).start()
    for h in range(2):
        yd(0, h).start()

    def forward(p):
        gx(1, p).wait_recv()
        gx(2, p).start()
        gy(1, p).wait_recv()
        gy(2, p).start()

    def land(g, h):
        kind = g - 1
        if kind != 1:
            for p in pieces_of(h):
                gx(kind, p).wait_recv()
                gy(kind, p).wait_recv()
        yd(g, h).start()

    order = [0, 1]

    def fresh(n):
        order.append(n)
        return [(n, m) for m in order[:-1]] + [(m, n) for m in order]

    for h in range(2):
        yd(0, h).wait_recv()
    logits_tile(0, 0, True)
    logits_tile(1, 1, True)
    logits_tiles([(0, 1), (1, 0)])
    forward(0)
    land(1, 0)
    forward(1)
    yd(1, 0).wait_recv()
    logits_tiles(fresh(2))
    forward(2)
    forward(3)
    land(2, 0)
    land(1, 1)
    yd(2, 0).wait_recv()
    yd(1, 1).wait_recv()
    wave = fresh(3) + fresh(4)
    logits_tiles(wave[:8])
    forward(4)
    logits_tiles(wave[8:])
    forward(5)
    land(3, 0)
    yd(3, 0).wait_recv()
    wave = fresh(6)
    logits_tiles(wave[:5])
    forward(6)
    logits_tiles(wave[5:])
    forward(7)
    land(2, 1)
    yd(2, 1).wait_recv()
    rest = fresh(5)
    now = [(5, 6), (6, 5), (5, 4), (4, 5)]
    logits_tiles(now)
    rest = [t for t in rest if t not in now]
    land(3, 1)
    yd(3, 1).wait_recv()
    rest += fresh(7)
    now = [(7, 6), (6, 7), (7, 4), (4, 7)]
    third = [(5, 2), (7, 2), (2, 5), (2, 7)]
    rest = [t for t in rest if t not in now + third]
    logits_tiles(now[:1])
    v_give(3, 0)
    logits_tiles(now[1:])
    v_take(3, 0)
    send_half(v_copy, 0, 0)
    d_copy(3, 0).wait_send()
    v_give(2, 0)
    u_sum(PU.at[0], 3, 0, 1)
    send_half(u_copy, 0, 0)
    v_take(2, 0)
    serve_v(0)
    u_sum(PU.at[1], 2, 0, 1)
    serve_u(0)
    logits_tiles(third)
    serve_v(1)
    serve_u(1)
    d_copy(2, 0).wait_send()
    v_give(1, 0)
    u_sum(PU.at[2], 1, 0, 1)
    send_half(u_copy, 1, 0)
    v_take(1, 0)
    send_half(v_copy, 1, 0)
    serve_v(2)
    serve_u(2)
    logits_tiles(rest[:4])
    serve_v(3)
    serve_u(3)
    logits_tiles(rest[4:])
    v_give(3, 1)
    u_sum(PU.at[0], 3, 1, 2)
    send_half(u_copy, 0, 1)
    v_take(3, 1)
    send_half(v_copy, 0, 1)
    d_copy(3, 1).wait_send()
    v_give(2, 1)
    u_sum(PU.at[1], 2, 1, 2)
    v_take(2, 1)

    rows_out = []
    for k in range(4):
        acc = jnp.sum(ST[k], axis=0, keepdims=True)
        tot = acc[:, :128]
        for m in range(1, acc.shape[1] // 128):
            tot = tot + acc[:, m * 128:(m + 1) * 128]
        rows_out.append(tot)
    SE[0] = jnp.concatenate(rows_out + [jnp.zeros((4, 128), F32)], axis=0)
    se_z = [remote(SE.at[0], SE.at[1 + k], se_s.at[k], se_r.at[k], dev) for k, dev in enumerate(z_peers)]
    se_p = [remote(SE.at[4], SE.at[5 + k], se_s.at[3 + k], se_r.at[3 + k], dev)
            for k, dev in enumerate(plane_peers)]

    for c in se_z:
        c.start()
    d_copy(2, 1).wait_send()
    v_give(1, 1)
    u_sum(PU.at[2], 1, 1, 2)
    send_half(u_copy, 1, 1)
    v_take(1, 1)
    send_half(v_copy, 1, 1)
    serve_v(4)
    serve_u(4)
    for h in range(2):
        d_copy(1, h).wait_send()
    v_sum(WV, 0, 1, 0, 2)
    serve_v(5)
    serve_u(5)

    def own_room(h):
        for p in pieces_of(h):
            v_copy(0, p).wait_send()
        pl.semaphore_signal(credit.at[h], inc=1, device_id=(partner,), device_id_type=MESH)
        pl.semaphore_wait(credit.at[h], 1)
        d_copy(0, h).start()
        for p in pieces_of(h):
            u_copy(0, p).wait_send()

    own_room(0)
    u_sum(PU.at[0], 0, 0, 1)
    serve_v(6)
    serve_u(6)
    v_take(0, 0)
    serve_v(7)
    serve_u(7)
    own_room(1)
    u_sum(PU.at[0], 0, 1, 2)
    for c in se_z:
        c.wait_recv()
    SE[4] = SE[0] + SE[1] + SE[2] + SE[3]
    for c in se_p:
        c.start()
    v_take(0, 1)
    for p in range(PIECES):
        for kind in range(3):
            gx(kind, p).wait_send()
            gy(kind, p).wait_send()
    for g in range(4):
        for h in range(2):
            yd(g, h).wait_send()
    raw_x = pltpu.make_async_copy(img_hbm, X.at[pl.ds(rows, rows)], ld_sem.at[0])
    raw_y = pltpu.make_async_copy(txt_hbm, X.at[pl.ds(2 * rows, rows)], ld_sem.at[1])
    raw_x.start()
    raw_y.start()
    raw_x.wait()
    raw_y.wait()
    temp = scal[0]

    def finish(copy, slots, part, raw_row, out, p, sem):
        copy(1, p).wait_recv()
        copy(2, p).wait_recv()
        blk = min(32, piece)

        def body(k, carry):
            at = p * piece + k * blk
            sl = pl.ds(pl.multiple_of(at, blk), blk)
            e32 = X[pl.ds(pl.multiple_of(raw_row + at, blk), blk), :].astype(F32)
            inv = lax.rsqrt(jnp.sum(e32 * e32, axis=-1, keepdims=True))
            unit = e32 * inv
            grad = (slots[1, sl, :] + part[1, sl, :] + part[0, sl, :]) * temp
            radial = jnp.sum(unit * grad, axis=-1, keepdims=True)
            slots[1, sl, :] = (grad - unit * radial) * inv
            return carry

        lax.fori_loop(0, piece // blk, body, 0)
        return pltpu.make_async_copy(slots.at[1, prow(p)], out.at[prow(p)], sem)

    outs = []
    for p in range(PIECES):
        outs.append(finish(u_copy, RU, PU, rows, u_out, p, out_sem.at[len(outs)]))
        outs[-1].start()
    for p in range(PIECES):
        outs.append(finish(v_copy, RV, DV, 2 * rows, v_out, p, out_sem.at[len(outs)]))
        outs[-1].start()
    for c in se_p:
        c.wait_recv()
    total = SE[4]
    for k in range(7):
        total = total + SE[5 + k]
    stat_out[...] = jnp.broadcast_to(jnp.sum(total, axis=1, keepdims=True), stat_out.shape)
    for p in range(PIECES):
        for kind in (1, 2):
            u_copy(kind, p).wait_send()
            v_copy(kind, p).wait_send()
    for h in range(2):
        d_copy(0, h).wait_send()
    for c in se_z + se_p:
        c.wait_send()
    for c in outs:
        c.wait()


def solution(mesh):
    n_dev = mesh.shape['dp']

    def local_fn(img_emb, txt_emb, log_temp, logit_bias):
        rows, width = img_emb.shape
        total_rows = rows * n_dev
        temp_scale = jnp.exp(log_temp)
        scal = jnp.stack([temp_scale, logit_bias])
        dma = pltpu.SemaphoreType.DMA
        any_spec = pl.BlockSpec(memory_space=pl.ANY)
        vmem = pltpu.VMEM
        grad_img, grad_txt, stats = pl.pallas_call(
            loss_kernel,
            name='siglip_pairs',
            out_shape=(jax.ShapeDtypeStruct((rows, width), F32), jax.ShapeDtypeStruct((rows, width), F32),
                       jax.ShapeDtypeStruct((8, 128), F32)),
            in_specs=[pl.BlockSpec(memory_space=pltpu.SMEM), any_spec, any_spec],
            out_specs=(any_spec, any_spec, pl.BlockSpec(memory_space=pltpu.VMEM)),
            scratch_shapes=[
                vmem((SQUARE * rows, width), BF16),
                vmem((2 * SQUARE * rows, width), BF16),
                vmem((SQUARE * rows, 2 * SQUARE * rows), BF16),
                vmem((3, rows, width), F32),
                vmem((2, rows, width), F32),
                vmem((3, rows, width), F32),
                vmem((rows, width), F32),
                vmem((2, rows, width), F32),
                vmem((4, 8, rows), F32),
                vmem((12, 8, 128), F32),
                dma((4,)), dma((3 * PIECES,)), dma((3 * PIECES,)), dma((3 * PIECES,)), dma((3 * PIECES,)),
                dma((8,)), dma((8,)),
                dma((3 * PIECES,)), dma((3 * PIECES,)), dma((3 * PIECES,)), dma((3 * PIECES,)),
                dma((8,)), dma((8,)), dma((10,)), dma((10,)), dma((2 * PIECES,)),
                pltpu.SemaphoreType.REGULAR((2,)),
                pltpu.SemaphoreType.REGULAR((PIECES,)), pltpu.SemaphoreType.REGULAR((PIECES,)),
            ],
            compiler_params=pltpu.CompilerParams(collective_id=0, has_side_effects=True,
                                                 vmem_limit_bytes=67_000_000),
        )(scal, img_emb, txt_emb)
        sums = stats[:, 0] / total_rows
        return sums[0] * LN2 + sums[3], grad_img, grad_txt, temp_scale * sums[2], sums[1]

    return jax.shard_map(
        local_fn,
        mesh=mesh,
        in_specs=(P('dp', None), P('dp', None), P(), P()),
        out_specs=(P(), P('dp', None), P('dp', None), P(), P()),
        check_vma=False,
    )
```

```python
import functools
import math

import jax
import jax.numpy as jnp
from jax import lax
from jax.experimental import pallas as pl
from jax.experimental.pallas import tpu as pltpu
from jax.sharding import PartitionSpec as P

F32 = jnp.float32
BF16 = jnp.bfloat16
MESH = pl.DeviceIdType.MESH
LOG2E = math.log2(math.e)
LN2 = math.log(2.0)
PLANE = 8
SQUARE = 4
PIECES = 8


def dot_f32(lhs, rhs, lhs_dim, rhs_dim):
    return lax.dot_general(lhs, rhs, (((lhs_dim,), (rhs_dim,)), ((), ())), preferred_element_type=F32)


def pick(table, idx):
    out = jnp.int32(table[0])
    for pos in range(1, len(table)):
        out = jnp.where(idx == pos, jnp.int32(table[pos]), out)
    return out


def loss_kernel(log_temp, logit_bias, img_hbm, txt_hbm, u_out, v_out, stat_out,
                X, Y, H, PU, RU, DV, WV, RV, ST, SE,
                ld_sem, gx_s, gx_r, gy_s, gy_r, yd_s, yd_r, ru_s, ru_r, rv_s, rv_r,
                dv_s, dv_r, se_s, se_r, out_sem, credit, uz_credit, vz_credit):
    rows, width = img_hbm.shape
    half = rows // 2
    piece = rows // PIECES
    me = lax.axis_index('dp')
    z = me // PLANE
    rem = me % PLANE
    y = rem // 4
    x = (rem // 2) % 2
    core = rem % 2
    x_dev = z * PLANE + rem + 2 - 4 * x
    y_dev = z * PLANE + rem + 4 - 8 * y
    lo_dev = (z + 1 - 2 * (z % 2)) * PLANE + rem
    hi_dev = ((z + 2) % 4) * PLANE + rem
    partner = me + 1 - 2 * core
    z_peers = [((z + k) % 4) * PLANE + rem for k in range(1, 4)]
    plane_peers = [z * PLANE + (rem + k) % PLANE for k in range(1, PLANE)]

    barrier = pltpu.get_barrier_semaphore()
    for dev in z_peers + plane_peers:
        pl.semaphore_signal(barrier, inc=1, device_id=(dev,), device_id_type=MESH)

    def xrow(g, r=0):
        return g * rows + r

    def yrow(g, r=0, other=0):
        return g * 2 * rows + (r // half) * rows + other * half + r % half

    loads = []
    for h in range(2):
        loads.append(pltpu.make_async_copy(img_hbm.at[pl.ds(h * half, half)], X.at[pl.ds(h * half, half)],
                                           ld_sem.at[h]))
        loads.append(pltpu.make_async_copy(txt_hbm.at[pl.ds(h * half, half)], Y.at[pl.ds(yrow(0, h * half), half)],
                                           ld_sem.at[2 + h]))
    for c in loads:
        c.start()
    ST[...] = jnp.zeros_like(ST)

    def normalize(ref, row):
        blk = min(64, half)

        def body(k, carry):
            sl = pl.ds(pl.multiple_of(row + k * blk, blk), blk)
            e32 = ref[sl, :].astype(F32)
            ref[sl, :] = (e32 * lax.rsqrt(jnp.sum(e32 * e32, axis=-1, keepdims=True))).astype(BF16)
            return carry

        lax.fori_loop(0, half // blk, body, 0)

    def remote(src, dst, ss, rs, dev):
        return pltpu.make_async_remote_copy(src_ref=src, dst_ref=dst, send_sem=ss, recv_sem=rs,
                                            device_id=(dev,), device_id_type=MESH)

    def gather(ref, row_of, ss, rs, flat_dev, z_dev, kind, p):
        src, dst = ((0, 1), (0, 2), (2, 3))[kind]
        n = kind * PIECES + p
        return remote(ref.at[pl.ds(row_of(src, p * piece), piece)], ref.at[pl.ds(row_of(dst, p * piece), piece)],
                      ss.at[n], rs.at[n], z_dev if kind == 1 else flat_dev)

    def gx(kind, p):
        return gather(X, xrow, gx_s, gx_r, x_dev, lo_dev, kind, p)

    def gy(kind, p):
        return gather(Y, yrow, gy_s, gy_r, y_dev, hi_dev, kind, p)

    def yd(g, p):
        return remote(Y.at[pl.ds(yrow(g, p * piece), piece)], Y.at[pl.ds(yrow(g, p * piece, 1), piece)],
                      yd_s.at[g * PIECES + p], yd_r.at[g * PIECES + p], partner)

    def pieces_of(h):
        return range(h * PIECES // 2, (h + 1) * PIECES // 2)

    def other_core(g, h):
        for p in pieces_of(h):
            yd(g, p).wait_recv()

    temp = jnp.max(jnp.exp(jnp.full((8, 128), log_temp[0], F32)))
    temp2 = temp * LOG2E
    bias2 = logit_bias[0] * LOG2E

    def col_sum(val):
        return jnp.sum(val.reshape(val.shape[0] // 8, 8, val.shape[1]), axis=0)

    def logits_tile(i, j, diag=False):
        irow = pl.multiple_of(i * half, half)
        jrow = pl.multiple_of(j * rows, rows)
        sim = dot_f32(X[pl.ds(irow, half), :], Y[pl.ds(jrow, rows), :], 1, 1)
        lg = sim * temp2 + bias2
        ex = jnp.exp2(-jnp.abs(lg))
        rc = 1.0 / (1.0 + ex)
        er = ex * rc
        wt = jnp.where(lg >= 0.0, rc, er)
        ramp = jnp.maximum(lg, 0.0)
        if diag:
            same = (lax.broadcasted_iota(jnp.int32, sim.shape, 0)
                    == lax.broadcasted_iota(jnp.int32, sim.shape, 1))
            wt = jnp.where(same, -jnp.where(lg >= 0.0, er, rc), wt)
            ramp = jnp.where(same, jnp.maximum(-lg, 0.0), ramp)
        H[pl.ds(irow, half), pl.ds(jrow, rows)] = wt.astype(BF16)
        ST[0] += col_sum(ramp)
        ST[1] += col_sum(wt)
        ST[2] += col_sum(wt * sim)
        prod = ex
        while prod.shape[0] > 8:
            m = prod.shape[0] // 2
            a, b = prod[:m], prod[m:]
            prod = a + b + a * b
        ST[3] += jnp.log1p(prod)

    def logits_tiles(pairs, per_step=2):
        def body(k, carry):
            for n in range(per_step):
                part = pairs[n::per_step]
                logits_tile(pick([p[0] for p in part], k), pick([p[1] for p in part], k))
            return carry

        lax.fori_loop(0, len(pairs) // per_step, body, 0)

    def u_sum(dst, g, h_lo, h_hi):
        def body(k, carry):
            h = h_lo + k // 4
            out = pl.ds(pl.multiple_of(h * half, half), half)
            sl = pl.ds(pl.multiple_of((k % 4) * (2 * rows), 2 * rows), 2 * rows)

            @pl.when(k % 4 == 0)
            def _():
                dst[out, :] = jnp.zeros((half, width), F32)

            dst[out, :] += dot_f32(H[pl.ds(pl.multiple_of(g * rows + h * half, half), half), sl], Y[sl, :], 1, 0)
            return carry

        lax.fori_loop(0, 4 * (h_hi - h_lo), body, 0)

    def v_sum(dst, g, other, h_lo, h_hi):
        def body(k, carry):
            h = h_lo + k // 2
            out = pl.ds(pl.multiple_of(h * half, half), half)
            sl = pl.ds(pl.multiple_of((k % 2) * (2 * rows), 2 * rows), 2 * rows)
            if other:
                @pl.when(k % 2 == 0)
                def _():
                    dst[out, :] = jnp.zeros((half, width), F32)

            cols = pl.ds(pl.multiple_of(g * 2 * rows + h * rows + other * half, half), half)
            dst[out, :] += dot_f32(H[sl, cols], X[sl, :], 0, 0)
            return carry

        lax.fori_loop(0, 2 * (h_hi - h_lo), body, 0)

    def prow(p):
        return pl.ds(p * piece, piece)

    def reduce_copy(part, slots, ss, rs, flat_dev, z_dev, kind, p):
        src = (part.at[0], part.at[2], slots.at[0])[kind]
        dst = (slots.at[0], slots.at[1], part.at[1])[kind]
        n = kind * PIECES + p
        return remote(src.at[prow(p)], dst.at[prow(p)], ss.at[n], rs.at[n], z_dev if kind == 2 else flat_dev)

    def u_copy(kind, p):
        return reduce_copy(PU, RU, ru_s, ru_r, x_dev, lo_dev, kind, p)

    def v_copy(kind, p):
        return reduce_copy(DV, RV, rv_s, rv_r, y_dev, hi_dev, kind, p)

    def serve(copy, part, slots, free, z_dev, p):
        copy(0, p).wait_recv()
        slots[0, prow(p), :] += part[1, prow(p), :]
        pl.semaphore_signal(free.at[p], inc=1, device_id=(z_dev,), device_id_type=MESH)
        pl.semaphore_wait(free.at[p], 1)
        copy(2, p).start()

    def serve_u(p):
        serve(u_copy, PU, RU, uz_credit, lo_dev, p)

    def serve_v(p):
        serve(v_copy, DV, RV, vz_credit, hi_dev, p)

    slot_of = {3: 0, 2: 1, 1: 2, 0: 0}

    def d_copy(g, h):
        return remote(WV.at[pl.ds(h * half, half)], DV.at[slot_of[g], pl.ds(h * half, half)],
                      dv_s.at[2 * g + h], dv_r.at[2 * g + h], partner)

    quarter = half // 2

    def first_copy(n):
        sl = pl.ds(n * quarter, quarter)
        return remote(WV.at[sl], DV.at[0, sl], dv_s.at[8 + n], dv_r.at[8 + n], partner)

    def first_sum(dst, n, other):
        out = pl.ds(n * quarter, quarter)
        cols = pl.ds(yrow(3, n * quarter, other), quarter)
        val = dot_f32(H[:, cols], X[...], 0, 0)
        if other:
            dst[out, :] = val
        else:
            dst[out, :] += val

    def v_give(g, h):
        v_sum(WV, g, 1, h, h + 1)
        d_copy(g, h).start()

    def v_take(g, h):
        d_copy(g, h).wait_recv()
        v_sum(DV.at[slot_of[g]], g, 0, h, h + 1)

    def send_half(copy, kind, h):
        for p in pieces_of(h):
            copy(kind, p).start()

    for h in range(2):
        loads[2 * h].wait()
        normalize(X, h * half)
        loads[2 * h + 1].wait()
        normalize(Y, yrow(0, h * half))
    pl.semaphore_wait(barrier, len(z_peers) + len(plane_peers))
    for p in range(PIECES):
        for kind in range(2):
            gx(kind, p).start()
            gy(kind, p).start()
    for p in range(PIECES):
        yd(0, p).start()

    def forward(p):
        gy(1, p).wait_recv()
        gy(2, p).start()
        yd(2, p).start()
        gx(1, p).wait_recv()
        gx(2, p).start()

    def land(g, h):
        for p in pieces_of(h):
            gy(g - 1, p).wait_recv()
            yd(g, p).start()
        for p in pieces_of(h):
            gx(g - 1, p).wait_recv()

    order = [0, 1]

    def fresh(n):
        order.append(n)
        return [(n, m) for m in order[:-1]] + [(m, n) for m in order]

    for h in range(2):
        other_core(0, h)
    logits_tile(0, 0, True)
    logits_tile(1, 1, True)
    logits_tiles([(0, 1), (1, 0)], 1)
    forward(0)
    land(1, 0)
    forward(1)
    other_core(1, 0)
    wave = fresh(2)
    logits_tiles(wave[:4], 1)
    wave = wave[4:]
    forward(2)
    forward(3)
    land(1, 1)
    other_core(2, 0)
    other_core(1, 1)
    wave += fresh(3) + fresh(4)
    logits_tiles(wave[:8], 1)
    forward(4)
    logits_tiles(wave[8:16], 1)
    forward(5)
    land(3, 0)
    other_core(3, 0)
    wave = wave[16:] + fresh(6)
    logits_tiles(wave[:6])
    forward(6)
    logits_tiles(wave[6:])
    forward(7)
    other_core(2, 1)
    rest = fresh(5)
    now = [(5, 6), (6, 5), (5, 4), (4, 5)]
    logits_tiles(now)
    rest = [t for t in rest if t not in now]
    land(3, 1)
    other_core(3, 1)
    rest += fresh(7)
    now = [(7, 6), (6, 7), (7, 4), (4, 7)]
    third = [(5, 2), (7, 2), (2, 5), (2, 7)]
    rest = [t for t in rest if t not in now + third]
    logits_tiles(now[:2])
    for n in range(2):
        first_sum(WV, n, 1)
        first_copy(n).start()
    for n in range(2):
        first_copy(n).wait_recv()
        first_sum(DV.at[0], n, 0)
        for p in range(n * PIECES // 4, (n + 1) * PIECES // 4):
            v_copy(0, p).start()
    u_sum(PU.at[0], 3, 0, 1)
    send_half(u_copy, 0, 0)
    logits_tiles(now[2:])
    for n in range(2):
        first_copy(n).wait_send()
    v_give(2, 0)
    v_take(2, 0)
    serve_v(0)
    u_sum(PU.at[1], 2, 0, 1)
    serve_u(0)
    logits_tiles(third)
    d_copy(2, 0).wait_send()
    v_give(1, 0)
    serve_v(1)
    v_take(1, 0)
    send_half(v_copy, 1, 0)
    serve_u(1)
    u_sum(PU.at[2], 1, 0, 1)
    send_half(u_copy, 1, 0)
    serve_v(2)
    serve_u(2)
    logits_tiles(rest[:4])
    serve_v(3)
    serve_u(3)
    logits_tiles(rest[4:])
    v_give(3, 1)
    u_sum(PU.at[0], 3, 1, 2)
    send_half(u_copy, 0, 1)
    v_take(3, 1)
    send_half(v_copy, 0, 1)
    d_copy(3, 1).wait_send()
    v_give(2, 1)
    u_sum(PU.at[1], 2, 1, 2)
    v_take(2, 1)

    rows_out = []
    for k in range(4):
        acc = jnp.sum(ST[k], axis=0, keepdims=True)
        tot = acc[:, :128]
        for m in range(1, acc.shape[1] // 128):
            tot = tot + acc[:, m * 128:(m + 1) * 128]
        rows_out.append(tot)
    SE[0] = jnp.concatenate(rows_out + [jnp.zeros((4, 128), F32)], axis=0)
    se_z = [remote(SE.at[0], SE.at[1 + k], se_s.at[k], se_r.at[k], dev) for k, dev in enumerate(z_peers)]
    se_p = [remote(SE.at[4], SE.at[5 + k], se_s.at[3 + k], se_r.at[3 + k], dev)
            for k, dev in enumerate(plane_peers)]

    for c in se_z:
        c.start()
    d_copy(2, 1).wait_send()
    v_give(1, 1)
    serve_v(4)
    v_take(1, 1)
    send_half(v_copy, 1, 1)
    u_sum(PU.at[2], 1, 1, 2)
    send_half(u_copy, 1, 1)
    serve_u(4)
    for h in range(2):
        d_copy(1, h).wait_send()
    v_sum(WV, 0, 1, 0, 2)
    serve_v(5)
    serve_u(5)

    def own_room(h):
        for p in pieces_of(h):
            v_copy(0, p).wait_send()
        pl.semaphore_signal(credit.at[h], inc=1, device_id=(partner,), device_id_type=MESH)
        pl.semaphore_wait(credit.at[h], 1)
        d_copy(0, h).start()
        for p in pieces_of(h):
            u_copy(0, p).wait_send()

    own_room(0)
    u_sum(PU.at[0], 0, 0, 1)
    serve_v(6)
    serve_u(6)
    v_take(0, 0)
    serve_v(7)
    serve_u(7)
    own_room(1)
    u_sum(PU.at[0], 0, 1, 2)
    for c in se_z:
        c.wait_recv()
    SE[4] = SE[0] + SE[1] + SE[2] + SE[3]
    for c in se_p:
        c.start()
    v_take(0, 1)
    for p in range(PIECES):
        for kind in range(3):
            gx(kind, p).wait_send()
            gy(kind, p).wait_send()
    for g in range(4):
        for p in range(PIECES):
            yd(g, p).wait_send()
    raw_x = pltpu.make_async_copy(img_hbm, X.at[pl.ds(rows, rows)], ld_sem.at[0])
    raw_y = pltpu.make_async_copy(txt_hbm, X.at[pl.ds(2 * rows, rows)], ld_sem.at[1])
    raw_x.start()
    raw_y.start()
    raw_x.wait()
    raw_y.wait()

    def finish(copy, slots, part, raw_row, out, p, sem):
        copy(1, p).wait_recv()
        copy(2, p).wait_recv()
        blk = min(32, piece)

        def body(k, carry):
            at = p * piece + k * blk
            sl = pl.ds(pl.multiple_of(at, blk), blk)
            e32 = X[pl.ds(pl.multiple_of(raw_row + at, blk), blk), :].astype(F32)
            inv = lax.rsqrt(jnp.sum(e32 * e32, axis=-1, keepdims=True))
            unit = e32 * inv
            grad = (slots[1, sl, :] + part[1, sl, :] + part[0, sl, :]) * temp
            radial = jnp.sum(unit * grad, axis=-1, keepdims=True)
            slots[1, sl, :] = (grad - unit * radial) * inv
            return carry

        lax.fori_loop(0, piece // blk, body, 0)
        return pltpu.make_async_copy(slots.at[1, prow(p)], out.at[prow(p)], sem)

    outs = []
    for p in range(PIECES):
        outs.append(finish(u_copy, RU, PU, rows, u_out, p, out_sem.at[len(outs)]))
        outs[-1].start()
    for p in range(PIECES):
        outs.append(finish(v_copy, RV, DV, 2 * rows, v_out, p, out_sem.at[len(outs)]))
        outs[-1].start()
    for c in se_p:
        c.wait_recv()
    total = SE[4]
    for k in range(7):
        total = total + SE[5 + k]
    stat_out[...] = jnp.broadcast_to(jnp.sum(total, axis=1, keepdims=True), stat_out.shape)
    for p in range(PIECES):
        for kind in (1, 2):
            u_copy(kind, p).wait_send()
            v_copy(kind, p).wait_send()
    for h in range(2):
        d_copy(0, h).wait_send()
    for c in se_z + se_p:
        c.wait_send()
    for c in outs:
        c.wait()


def solution(mesh):
    n_dev = mesh.shape['dp']

    def local_fn(img_emb, txt_emb, log_temp, logit_bias):
        rows, width = img_emb.shape
        total_rows = rows * n_dev
        temp_scale = jnp.exp(log_temp)
        dma = pltpu.SemaphoreType.DMA
        any_spec = pl.BlockSpec(memory_space=pl.ANY)
        vmem = pltpu.VMEM
        grad_img, grad_txt, stats = pl.pallas_call(
            loss_kernel,
            name='siglip_pairs',
            out_shape=(jax.ShapeDtypeStruct((rows, width), F32), jax.ShapeDtypeStruct((rows, width), F32),
                       jax.ShapeDtypeStruct((8, 128), F32)),
            in_specs=[pl.BlockSpec(memory_space=pltpu.SMEM)] * 2 + [any_spec] * 2,
            out_specs=(any_spec, any_spec, pl.BlockSpec(memory_space=pltpu.VMEM)),
            scratch_shapes=[
                vmem((SQUARE * rows, width), BF16),
                vmem((2 * SQUARE * rows, width), BF16),
                vmem((SQUARE * rows, 2 * SQUARE * rows), BF16),
                vmem((3, rows, width), F32),
                vmem((2, rows, width), F32),
                vmem((3, rows, width), F32),
                vmem((rows, width), F32),
                vmem((2, rows, width), F32),
                vmem((4, 8, rows), F32),
                vmem((12, 8, 128), F32),
                dma((4,)), dma((3 * PIECES,)), dma((3 * PIECES,)), dma((3 * PIECES,)), dma((3 * PIECES,)),
                dma((4 * PIECES,)), dma((4 * PIECES,)),
                dma((3 * PIECES,)), dma((3 * PIECES,)), dma((3 * PIECES,)), dma((3 * PIECES,)),
                dma((10,)), dma((10,)), dma((10,)), dma((10,)), dma((2 * PIECES,)),
                pltpu.SemaphoreType.REGULAR((2,)),
                pltpu.SemaphoreType.REGULAR((PIECES,)), pltpu.SemaphoreType.REGULAR((PIECES,)),
            ],
            compiler_params=pltpu.CompilerParams(collective_id=0, has_side_effects=True,
                                                 vmem_limit_bytes=67_000_000),
        )(log_temp.reshape(1), logit_bias.reshape(1), img_emb, txt_emb)
        sums = stats[:, 0] / total_rows
        return sums[0] * LN2 + sums[3], grad_img, grad_txt, temp_scale * sums[2], sums[1]

    return jax.shard_map(
        local_fn,
        mesh=mesh,
        in_specs=(P('dp', None), P('dp', None), P(), P()),
        out_specs=(P(), P('dp', None), P('dp', None), P(), P()),
        check_vma=False,
    )
```
